256 devices in a mesh: section: 8 (over x, core), dp: 32 (over y, z).
Axes of the slice: x: 4, y: 4, z: 8, core: 2. Of those that a mesh axis runs over, the one named last changes fastest.
Arguments:
- item_owner: int32 [8, 32, 128, 1], P('section', 'dp'), may hold values from 0 to 31; in each aligned block of 128 rows (0 to 127, 128 to 255, ..., all dimensions but the last counted through in order) at most 8 rows name the same one
- item_row: int32 [8, 32, 128], P('section', 'dp'), may hold values from 0 to 255
- lengths: int32 [8, 32], P(None, 'dp'), may hold values from 1 to 128
- table: bfloat16 [8192, 1024], P('dp'), may hold values from -6 to 6
- w_in: bfloat16 [8, 1024, 4096], P('section', 'dp'), may hold values from -0.1875 to 0.1875
- w_out: bfloat16 [8, 1024, 1024], P('section', 'dp'), may hold values from -0.1875 to 0.1875
- gain_in: float32 [8, 1024], P('section'), may hold values from 0.5 to 1.5
- gain_mid: float32 [8, 1024], P('section'), may hold values from 0.5 to 1.5
Outputs:
- states: bfloat16 [8, 32, 8, 128, 1024], P('section', 'dp')
The draws below stay inside these ranges and needn't reach their ends.
Inputs may be any that keep to these rules, and one draw needn't show every extreme that they name: Among the 128 events of one history no value of item_owner appears more than 8 times; some history reaches 8.
All inputs are finite; a program needn't handle non-finite values.
Results may differ from the reference program's by a relative error of at most 0.029.
Values may be sent and summed in bfloat16 or wider, within the bound.
No kernel may reach another device: no remote copies, remote signals or barrier semaphores. Data moves between devices by JAX's collectives and lax.ppermute only.
A program may use at most 64 MiB of HBM per device.

```python
import math
import jax
import jax.numpy as jnp
import numpy as np
from jax import lax

D = 1024
HEADS = 8
HEAD_DIM = 128
LEN = 128
ROWS_DEV = 256
MICRO = 8
GROUPS = 32
ITEMS = 8192
CAP = 8
N_SECTION = 8
N_DP = 32


def set_ends(values, rng, smallest, top_value):
    longest = values.shape.index(max(values.shape))
    spots = []
    for shift in (0, 1):
        where = [jax.random.randint(jax.random.fold_in(rng, axis), (), 0, length) for axis, length in enumerate(values.shape)]
        where[longest] = (where[longest] + shift) % values.shape[longest]
        spots.append(tuple(where))
    return values.at[spots[0]].set(smallest).at[spots[1]].set(top_value)


def block_scale(key, dims, shards, low, high):
    factor_of, own = 1.0, jax.random.fold_in(key, 6)
    for dim, shards_of in shards:
        draws = jnp.exp(jax.random.uniform(jax.random.fold_in(own, dim), (shards_of,), jnp.float32, low / len(shards), high / len(shards)))
        factor_of = factor_of * jnp.repeat(draws, dims[dim] // shards_of).reshape([-1 if axis == dim else 1 for axis in range(len(dims))])
    return factor_of


def shared_out(key, own, number, rows, number_of, top, limit, lean):
    order = jax.random.permutation(key, number_of)
    packed, common = load_shares(number_of, rows * top, limit, lean, True), load_shares(number_of, rows * top, limit, lean, False)
    places = jnp.arange(number_of)

    def named(sizes, offset_by):
        used = int((sizes > 0).sum())
        fixed = max(1, used // 4)
        shifted = fixed + (places - fixed + offset_by * (used - fixed)) % max(1, number_of - fixed)
        return jnp.zeros((number_of,), jnp.int32).at[order[jnp.where(places < fixed, places, shifted)]].set(jnp.asarray(sizes, jnp.int32))

    sizes = jnp.where(number % 4 == 0, named(packed, number // 4), named(common, number - number // 4 - 1))
    mixed = jax.random.permutation(jax.random.fold_in(own, 3), number_of)
    giver, sink = mixed[0:number_of // 2 * 2:2], mixed[1:number_of // 2 * 2:2]
    slack = jnp.minimum(sizes[giver] - 1, limit - sizes[sink]) // 2
    slack = jnp.where((giver == order[0]) | (sink == order[0]) | (sizes[sink] == 0), 0, jnp.maximum(slack, 0))
    shifted = jax.random.randint(jax.random.fold_in(own, 4), (number_of // 2,), 0, 1 << 20) % (slack + 1)
    sizes = sizes.at[giver].add(-shifted).at[sink].add(shifted)
    items = jnp.searchsorted(jnp.cumsum(sizes), jnp.arange(rows * top), side="right").astype(jnp.int32)
    listing = items.reshape(top, rows).T
    listing = listing[jax.random.permutation(jax.random.fold_in(own, 1), rows)]
    offset_by = jax.random.randint(jax.random.fold_in(own, 2), (rows, 1), 0, top)
    return jnp.take_along_axis(listing, (jnp.arange(top)[None, :] + offset_by) % top, axis=1)


def load_shares(count, total, limit, lean, full):
    loads = [(1 << 20) // math.isqrt(standing ** lean) + 1 for standing in range(1, count + 1)]
    largest = limit if full else min(limit, max(-(-total // count), total * loads[0] // sum(loads)))
    least = 1 if total - largest >= count - 1 else 0
    counts, surplus = [largest] + [least] * (count - 1), total - largest - least * (count - 1)
    while surplus > 0:
        candidates = [i for i in range(1, count) if counts[i] < largest] or [i for i in range(1, count) if counts[i] < limit]
        pool, left = sum([loads[i] for i in candidates]), surplus
        for i in candidates:
            addition = min(limit - counts[i], max(1, left * loads[i] // pool), surplus)
            counts[i] = counts[i] + addition
            surplus = surplus - addition
    return np.array(counts)


def scatter_about(own_key, dims, width, bound, shards=(), kind=jnp.bfloat16):
    values = jax.random.normal(own_key, dims, jnp.float32) * width
    if len(shards) > 0:
        values = block_scale(own_key, dims, shards, -0.22, 0.18) * values
    return jnp.clip(values, min=-bound, max=bound).astype(kind)


def setup_inputs(seed: int = 0) -> dict:
    key_list = jax.random.split(jax.random.key(seed), 9)
    item_owner_keys = jax.random.split(jax.random.fold_in(key_list[0], 1), MICRO * GROUPS * LEN // LEN)
    item_owner_turns = jax.random.permutation(jax.random.fold_in(key_list[0], 3), MICRO * GROUPS * LEN // LEN)
    item_owner = jax.vmap(lambda own, number: shared_out(jax.random.fold_in(key_list[0], 2), own, number, LEN, N_DP, 1, CAP, 1))(item_owner_keys, item_owner_turns).reshape((MICRO, GROUPS, LEN, 1))
    item_row = set_ends(jax.random.randint(key_list[1], (MICRO, GROUPS, LEN), 0, ROWS_DEV), jax.random.fold_in(key_list[1], 1), 0, ROWS_DEV - 1).astype(jnp.int32)
    lengths = set_ends(jax.random.randint(key_list[2], (MICRO, GROUPS), 1, LEN + 1), jax.random.fold_in(key_list[2], 1), 1, LEN).astype(jnp.int32)
    table = scatter_about(key_list[3], (ITEMS, D), 1.0, 6.0, ((0, 32),))
    w_in = scatter_about(key_list[4], (N_SECTION, D, 4 * D), D ** -0.5, 0.1875, ((0, 8), (1, 32)))
    w_out = scatter_about(key_list[5], (N_SECTION, D, D), D ** -0.5, 0.1875, ((0, 8), (1, 32)))
    gain_in = jnp.clip(1.0 + 0.1 * jax.random.normal(key_list[6], (N_SECTION, D), jnp.float32), 0.5, 1.5)
    gain_mid = jnp.clip(1.0 + 0.1 * jax.random.normal(key_list[7], (N_SECTION, D), jnp.float32), 0.5, 1.5)
    return dict(item_owner=item_owner, item_row=item_row, lengths=lengths, table=table, w_in=w_in, w_out=w_out, gain_in=gain_in, gain_mid=gain_mid)


EPS = 1e-05

def normalize(values):
    center = values - lax.optimization_barrier(jnp.mean(values, axis=-1, keepdims=True))
    spread = lax.optimization_barrier(jnp.mean(center * center, axis=-1, keepdims=True))
    return center * lax.rsqrt(spread + EPS)

def hstu_layer(current, length, weight_in, weight_out, scale_in, scale_mid):
    wide = current.astype(jnp.float32)
    normed = (normalize(wide) * scale_in).astype(jnp.bfloat16)
    uvqk = jax.nn.silu(jnp.dot(normed, weight_in, preferred_element_type=jnp.float32)).astype(jnp.bfloat16)
    u_part, v_part, q_part, k_part = jnp.split(uvqk, 4, axis=-1)
    rows = current.shape[0]
    queries = q_part.reshape(rows, HEADS, HEAD_DIM).astype(jnp.float32)
    keys = k_part.reshape(rows, HEADS, HEAD_DIM).astype(jnp.float32)
    values = v_part.reshape(rows, HEADS, HEAD_DIM).astype(jnp.float32)
    scores = jnp.einsum('qhd,khd->hqk', queries, keys)
    position = jnp.arange(rows, dtype=jnp.int32)
    allowed = (position[None, :] <= position[:, None]) & (position[None, :] < length)
    weights = jnp.where(allowed[None], jax.nn.silu(scores / jnp.sqrt(jnp.float32(HEAD_DIM))), 0.0).astype(jnp.bfloat16)
    attn = jnp.einsum('hqk,khd->qhd', weights.astype(jnp.float32), values).reshape(rows, HEADS * HEAD_DIM)
    mixed = (normalize(attn) * scale_mid * u_part.astype(jnp.float32)).astype(jnp.bfloat16)
    return (jnp.dot(mixed, weight_out, preferred_element_type=jnp.float32) + wide).astype(jnp.bfloat16)

def reference(item_owner, item_row, lengths, table, w_in, w_out, gain_in, gain_mid):
    sections = w_in.shape[0]
    micro, groups, seq_len = item_row.shape
    index = (item_owner[..., 0] * ROWS_DEV + item_row).astype(jnp.int32).reshape(micro * groups, seq_len)
    lens = lengths.reshape(micro * groups).astype(jnp.int32)

    def one_history(pair):
        rows, length = pair
        current = jnp.take(table, rows, axis=0)
        kept = []
        for level in range(sections):
            current = hstu_layer(current, length, w_in[level], w_out[level], gain_in[level], gain_mid[level])
            kept.append(current)
        return jnp.stack(kept)
    result = lax.map(one_history, (index, lens))
    result = result.reshape(micro, groups, sections, seq_len, table.shape[1])
    return jnp.transpose(result, (2, 1, 0, 3, 4))
```

```python
import functools

import jax
import jax.numpy as jnp
from jax import lax
from jax.experimental import pallas as pl
from jax.experimental.pallas import tpu as pltpu
from jax.sharding import Mesh
from jax.sharding import PartitionSpec as P

HEADS = 8
HEAD = 128
WIDTH = 1024
ROWS = 128
PAIR = 2 * HEAD
EPS = 1e-05
STAGES = 4
SHARE = 4
DP = ("dp_0", "dp_1")
ALL = ("chip", "core")


def silu(values):
    half = 0.5 * values
    return half + half * jnp.tanh(half)


def normalize(values):
    center = values - jnp.mean(values, axis=-1, keepdims=True)
    spread = jnp.mean(center * center, axis=-1, keepdims=True)
    return center * lax.rsqrt(spread + EPS)


def stage_kernel(
    step_ref,
    info_ref,
    inputs_ref,
    incoming_ref,
    mine_ref,
    other_ref,
    gain_in_ref,
    gain_mid_ref,
    out_in,
    send_in,
    out_ref,
    send_ref,
    next_ref,
    weights,
    current,
    projected,
    results,
    weight_sems,
    out_sem,
    in_sem,
):
    core = info_ref[8]
    chip = info_ref[9]
    which = step_ref[0] - 2 * chip
    pairs = HEADS // 2

    def columns(part):
        if part == pairs:
            return [pl.ds(4 * WIDTH, WIDTH)]
        return [pl.ds(block * WIDTH + part * PAIR, PAIR) for block in range(4)]

    def fetch(source, section, part):
        return [
            pltpu.make_async_copy(
                source.at[:, cols], weights.at[section, :, cols], weight_sems.at[section, part, k]
            )
            for k, cols in enumerate(columns(part))
        ]

    @pl.when((which >= 0) & (which < SHARE))
    def _():
        @pl.when(chip == 0)
        def _():
            pltpu.make_async_copy(inputs_ref.at[which], current, in_sem).start()

        @pl.when(chip != 0)
        def _():
            pltpu.make_async_copy(incoming_ref, current, in_sem).start()

        for section in range(2):

            @pl.when(core == section)
            def _():
                for part in range(pairs + 1):
                    for copy in fetch(mine_ref, section, part):
                        copy.start()

            @pl.when(core != section)
            def _():
                for part in range(pairs + 1):
                    for copy in fetch(other_ref, section, part):
                        copy.start()

        length = info_ref[2 * which + core]
        row = lax.broadcasted_iota(jnp.int32, (ROWS, ROWS), 0)
        col = lax.broadcasted_iota(jnp.int32, (ROWS, ROWS), 1)
        allowed = (col <= row) & (col < length)
        pltpu.make_async_copy(incoming_ref, current, in_sem).wait()

        for section in range(2):
            block = current[...] if section == 0 else results[0]
            wide = block.astype(jnp.float32)
            normed = (normalize(wide) * gain_in_ref[pl.ds(section, 1), :]).astype(jnp.bfloat16)
            heads = []
            for part in range(pairs):
                for copy in fetch(mine_ref, section, part):
                    copy.wait()
                q_k_v = []
                for index in (2, 3, 1, 0):
                    cols = columns(part)[index]
                    value = silu(
                        jnp.dot(
                            normed,
                            weights[section, :, cols],
                            preferred_element_type=jnp.float32,
                        )
                    ).astype(jnp.bfloat16)
                    if index == 0:
                        projected[:, pl.ds(part * PAIR, PAIR)] = value
                    else:
                        q_k_v.append(value)
                queries, keys, values = q_k_v
                for head in range(2):
                    at = slice(head * HEAD, (head + 1) * HEAD)
                    scores = lax.dot_general(
                        queries[:, at],
                        keys[:, at],
                        (((1,), (1,)), ((), ())),
                        preferred_element_type=jnp.float32,
                    )
                    weight = jnp.where(allowed, silu(scores * (HEAD**-0.5)), 0.0)
                    heads.append(
                        jnp.dot(
                            weight.astype(jnp.bfloat16),
                            values[:, at],
                            preferred_element_type=jnp.float32,
                        )
                    )
            attn = jnp.concatenate(heads, axis=1)
            mixed = normalize(attn) * gain_mid_ref[pl.ds(section, 1), :]
            mixed = (mixed * projected[...].astype(jnp.float32)).astype(jnp.bfloat16)
            for copy in fetch(mine_ref, section, pairs):
                copy.wait()
            result = jnp.dot(
                mixed,
                weights[section, :, pl.ds(4 * WIDTH, WIDTH)],
                preferred_element_type=jnp.float32,
            )
            result = (result + wide).astype(jnp.bfloat16)
            results[section] = result
            if section == 1:
                next_ref[...] = result

            @pl.when(core == section)
            def _():
                pltpu.make_async_copy(
                    results.at[section], out_ref.at[2 * which + core], out_sem.at[section]
                ).start()

            @pl.when(core != section)
            def _():
                pltpu.make_async_copy(
                    results.at[section], send_ref.at[which], out_sem.at[section]
                ).start()

        for section in range(2):
            pltpu.make_async_copy(
                results.at[section], send_ref.at[which], out_sem.at[section]
            ).wait()


def stage(step, info, inputs, incoming, mine, other, gain_in, gain_mid, out, send):
    smem = pl.BlockSpec(memory_space=pltpu.SMEM)
    vmem = pl.BlockSpec(memory_space=pltpu.VMEM)
    anywhere = pl.BlockSpec(memory_space=pl.ANY)
    block = jax.ShapeDtypeStruct((ROWS, WIDTH), jnp.bfloat16)
    return pl.pallas_call(
        stage_kernel,
        out_shape=(
            jax.ShapeDtypeStruct(out.shape, out.dtype),
            jax.ShapeDtypeStruct(send.shape, send.dtype),
            block,
        ),
        in_specs=[smem, smem, anywhere, anywhere, anywhere, anywhere, vmem, vmem, anywhere, anywhere],
        out_specs=(anywhere, anywhere, vmem),
        scratch_shapes=[
            pltpu.VMEM((2, WIDTH, 5 * WIDTH), jnp.bfloat16),
            pltpu.VMEM((ROWS, WIDTH), jnp.bfloat16),
            pltpu.VMEM((ROWS, WIDTH), jnp.bfloat16),
            pltpu.VMEM((2, ROWS, WIDTH), jnp.bfloat16),
            pltpu.SemaphoreType.DMA((2, HEADS // 2 + 1, 4)),
            pltpu.SemaphoreType.DMA((2,)),
            pltpu.SemaphoreType.DMA,
        ],
        input_output_aliases={8: 0, 9: 1},
        compiler_params=pltpu.CompilerParams(vmem_limit_bytes=40 * 1024 * 1024),
        cost_estimate=pl.CostEstimate(
            flops=2 * 2 * ROWS * WIDTH * 5 * WIDTH,
            bytes_accessed=2 * 2 * WIDTH * 5 * WIDTH,
            transcendentals=2 * ROWS * 5 * WIDTH,
        ),
    )(step, info, inputs, incoming, mine, other, gain_in, gain_mid, out, send)


def place_kernel(info_ref, received, out_in, out_ref, sems):
    core = info_ref[8]
    copies = [
        pltpu.make_async_copy(received.at[j], out_ref.at[2 * j + 1 - core], sems.at[j])
        for j in range(SHARE)
    ]
    for copy in copies:
        copy.start()
    for copy in copies:
        copy.wait()


def place(info, received, out):
    return pl.pallas_call(
        place_kernel,
        out_shape=jax.ShapeDtypeStruct(out.shape, out.dtype),
        in_specs=[
            pl.BlockSpec(memory_space=pltpu.SMEM),
            pl.BlockSpec(memory_space=pltpu.VMEM),
            pl.BlockSpec(memory_space=pl.ANY),
        ],
        out_specs=pl.BlockSpec(memory_space=pl.ANY),
        scratch_shapes=[pltpu.SemaphoreType.DMA((SHARE,))],
        input_output_aliases={2: 0},
        compiler_params=pltpu.CompilerParams(vmem_limit_bytes=8 * 1024 * 1024),
    )(info, received, out)


def lookup_items(item_owner, item_row, table):
    groups = lax.axis_size(DP)
    owner = item_owner.reshape(-1)
    rows = item_row.reshape(-1)
    seq_len = rows.shape[0]
    slots_each = max(2, 2 * seq_len // groups)
    match = (owner[:, None] == jnp.arange(groups, dtype=jnp.int32)[None, :]).astype(jnp.int32)
    earlier = jnp.cumsum(match, axis=0) - match
    slot = jnp.sum(earlier * match, axis=1)
    placed = match[:, :, None] * (
        slot[:, None, None] == jnp.arange(slots_each, dtype=jnp.int32)[None, None, :]
    ).astype(jnp.int32)
    request = jnp.sum(placed * rows[:, None, None], axis=0)
    received = lax.all_to_all(request, DP, split_axis=0, concat_axis=0, tiled=True)
    found = jnp.take(table, received.reshape(-1), axis=0, mode="clip")
    answered = lax.all_to_all(
        found.reshape(groups, slots_each, -1), DP, split_axis=0, concat_axis=0, tiled=True
    )
    flat_rows = answered.reshape(groups * slots_each, table.shape[1])
    return jnp.take(flat_rows, owner * slots_each + slot, axis=0, mode="clip")


def swap(block):
    return lax.ppermute(block, "core", [(0, 1), (1, 0)])


def on_device(item_owner, item_row, lengths, table, w_in, w_out, gain_in, gain_mid):
    core = lax.axis_index("core")
    chip = lax.axis_index("chip")
    shard = jnp.concatenate([w_in[0], w_out[0]], axis=1)
    mine = lax.all_gather(shard, DP, axis=0, tiled=True)
    embedded = lookup_items(item_owner, item_row, table)
    inputs = jnp.stack(
        [embedded] + [lax.ppermute(embedded, "chip", [(k, 0)]) for k in range(1, STAGES)]
    )
    gains = jnp.concatenate([gain_in, gain_mid], axis=0)
    gains_other = swap(gains)
    first = jnp.where(core == 0, gains, gains_other)
    second = jnp.where(core == 0, gains_other, gains)
    scale_in = jnp.stack([first[0], second[0]])
    scale_mid = jnp.stack([first[1], second[1]])
    other = swap(mine)
    info = jnp.concatenate(
        [lengths[:, 0], jnp.stack([core, chip]).astype(jnp.int32), jnp.zeros((6,), jnp.int32)]
    )
    blank = jnp.zeros((ROWS, WIDTH), jnp.bfloat16)
    out = jnp.zeros((2 * SHARE, ROWS, WIDTH), jnp.bfloat16)
    send = jnp.zeros((SHARE, ROWS, WIDTH), jnp.bfloat16)
    steps = SHARE + 2 * (STAGES - 1)
    forward = [(i, i + 1) for i in range(STAGES - 1)]

    def body(step, carry):
        out, send, previous, incoming = carry
        arriving = lax.ppermute(previous, "chip", forward)
        out, send, result = stage(
            step.reshape(1), info, inputs, incoming, mine, other, scale_in, scale_mid, out, send
        )
        return (out, send, result, arriving)

    out, send, _, _ = lax.fori_loop(0, steps, body, (out, send, blank, blank))
    out = place(info, swap(send), out)
    return out[None, None]


def solution(mesh):
    split = Mesh(mesh.devices.reshape(STAGES, 2, 4, 8), ("chip", "core", "dp_0", "dp_1"))
    placed = (
        P(ALL, DP, None, None),
        P(ALL, DP, None),
        P(None, DP),
        P(DP, None),
        P(ALL, DP, None),
        P(ALL, DP, None),
        P(ALL, None),
        P(ALL, None),
    )
    return jax.shard_map(
        on_device,
        mesh=split,
        in_specs=placed,
        out_specs=P(ALL, DP, None, None, None),
        check_vma=False,
    )
```

```python
import functools

import jax
import jax.numpy as jnp
from jax import lax
from jax.experimental import pallas as pl
from jax.experimental.pallas import tpu as pltpu
from jax.sharding import Mesh
from jax.sharding import PartitionSpec as P

HEADS = 8
HEAD = 128
WIDTH = 1024
ROWS = 128
PAIR = 2 * HEAD
EPS = 1e-05
STAGES = 4
SPLIT = 2
PIECES = 16
SOURCES = PIECES + 9
LEFT = SPLIT * WIDTH
RIGHT = 3 * WIDTH
SHARE = 4
DP = ("dp_0", "dp_1")
ALL = ("chip", "core")


def silu(values):
    half = 0.5 * values
    return half + half * jnp.tanh(half)


def normalize(values):
    center = values - jnp.mean(values, axis=-1, keepdims=True)
    spread = jnp.mean(center * center, axis=-1, keepdims=True)
    return center * lax.rsqrt(spread + EPS)


def stage_kernel(step_ref, info_ref, *refs):
    inputs_refs, incoming_ref, refs = refs[:STAGES], refs[STAGES], refs[STAGES + 1 :]
    mine_refs, sent_refs, refs = refs[:PIECES], refs[PIECES:SOURCES], refs[SOURCES:]
    other_refs = [None] * PIECES
    for ref, group in zip(sent_refs, GROUPS):
        for k, piece in enumerate(group):
            other_refs[piece] = ref if len(group) == 1 else ref.at[k]
    gain_in_ref, gain_mid_ref, _, _, out_ref, send_ref, next_ref = refs[:7]
    left, right, current, projected, results, weight_sems, out_sem, in_sem = refs[7:]
    core = info_ref[8]
    chip = info_ref[9]
    y, z = info_ref[10], info_ref[11]
    which = step_ref[0] - 2 * chip
    pairs = HEADS // 2

    def fetch(source, section):
        moves = []
        for part in range(SPLIT):
            cols = pl.ds(part * WIDTH, WIDTH)
            for k, d in enumerate(AROUND):
                place = left.at[section, :, lax.rem(z - d + 8, 8), :, cols]
                moves.append((source[k].at[:, :, cols], place, part * 8 + k))
        for k, d in enumerate(ROUND):
            for half in range(2):
                place = right.at[section, lax.rem(y - d + 4, 4), pl.ds(half * 4, 4)]
                n = 8 + 2 * k + half
                moves.append((source[n], place, 8 + n))
        return [pltpu.make_async_copy(a, b, weight_sems.at[section, n]) for a, b, n in moves]

    @pl.when((which >= 0) & (which < SHARE))
    def _():
        for k in range(STAGES):

            @pl.when((chip == 0) & (which == k))
            def _():
                pltpu.make_async_copy(inputs_refs[k], current, in_sem).start()

        @pl.when(chip != 0)
        def _():
            pltpu.make_async_copy(incoming_ref, current, in_sem).start()

        @pl.when(core == 0)
        def _():
            for copy in fetch(mine_refs, 0) + fetch(other_refs, 1):
                copy.start()

        @pl.when(core != 0)
        def _():
            for copy in fetch(other_refs, 0) + fetch(mine_refs, 1):
                copy.start()

        length = info_ref[2 * which + core]
        row = lax.broadcasted_iota(jnp.int32, (ROWS, ROWS), 0)
        col = lax.broadcasted_iota(jnp.int32, (ROWS, ROWS), 1)
        allowed = (col <= row) & (col < length)
        pltpu.make_async_copy(incoming_ref, current, in_sem).wait()

        def one_layer(section, carry):
            arrivals = fetch(mine_refs, section)
            wide = current[...].astype(jnp.float32)
            normed = (normalize(wide) * gain_in_ref[pl.ds(section, 1), :]).astype(jnp.bfloat16)
            heads = []
            for part in range(pairs):
                for copy in arrivals[part * 8 : part * 8 + 8] if part <= SPLIT else ():
                    copy.wait()
                q_k_v = []
                for index in (2, 3, 1, 0):
                    side, at = (left, part) if part < SPLIT else (right, part - SPLIT)
                    cols = pl.ds(at * WIDTH + index * PAIR, PAIR)
                    value = silu(
                        jnp.dot(
                            normed,
                            side[section, :, :, :, cols].reshape(WIDTH, PAIR),
                            preferred_element_type=jnp.float32,
                        )
                    ).astype(jnp.bfloat16)
                    if index == 0:
                        projected[:, pl.ds(part * PAIR, PAIR)] = value
                    else:
                        q_k_v.append(value)
                queries, keys, values = q_k_v
                for head in range(2):
                    at = slice(head * HEAD, (head + 1) * HEAD)
                    scores = lax.dot_general(
                        queries[:, at],
                        keys[:, at],
                        (((1,), (1,)), ((), ())),
                        preferred_element_type=jnp.float32,
                    )
                    weight = jnp.where(allowed, silu(scores * (HEAD**-0.5)), 0.0)
                    heads.append(
                        jnp.dot(
                            weight.astype(jnp.bfloat16),
                            values[:, at],
                            preferred_element_type=jnp.float32,
                        )
                    )
            attn = jnp.concatenate(heads, axis=1)
            mixed = normalize(attn) * gain_mid_ref[pl.ds(section, 1), :]
            mixed = (mixed * projected[...].astype(jnp.float32)).astype(jnp.bfloat16)
            result = jnp.dot(
                mixed,
                right[section, :, :, :, pl.ds(2 * WIDTH, WIDTH)].reshape(WIDTH, WIDTH),
                preferred_element_type=jnp.float32,
            )
            result = (result + wide).astype(jnp.bfloat16)
            results[section] = result
            current[...] = result

            @pl.when(core == section)
            def _():
                pltpu.make_async_copy(
                    results.at[section], out_ref.at[2 * which + core], out_sem.at[section]
                ).start()

            @pl.when(core != section)
            def _():
                pltpu.make_async_copy(
                    results.at[section], send_ref.at[which], out_sem.at[section]
                ).start()

            return carry

        lax.fori_loop(0, 2, one_layer, 0)
        onward = pltpu.make_async_copy(current, next_ref, in_sem)
        onward.start()
        for section in range(2):
            pltpu.make_async_copy(
                results.at[section], send_ref.at[which], out_sem.at[section]
            ).wait()
        onward.wait()


def stage(step, info, inputs, incoming, mine, other, gain_in, gain_mid, out, send):
    smem = pl.BlockSpec(memory_space=pltpu.SMEM)
    vmem = pl.BlockSpec(memory_space=pltpu.VMEM)
    hbm = pl.BlockSpec(memory_space=pltpu.HBM)
    block = jax.ShapeDtypeStruct((ROWS, WIDTH), jnp.bfloat16)
    return pl.pallas_call(
        stage_kernel,
        out_shape=(
            jax.ShapeDtypeStruct(out.shape, out.dtype),
            jax.ShapeDtypeStruct(send.shape, send.dtype),
            block,
        ),
        in_specs=[smem, smem]
        + [hbm] * (STAGES + 1 + SOURCES)
        + [vmem, vmem, hbm, hbm],
        out_specs=(hbm, hbm, hbm),
        scratch_shapes=[
            pltpu.VMEM((2, 4, 8, 32, LEFT), jnp.bfloat16),
            pltpu.VMEM((2, 4, 8, 32, RIGHT), jnp.bfloat16),
            pltpu.VMEM((ROWS, WIDTH), jnp.bfloat16),
            pltpu.VMEM((ROWS, WIDTH), jnp.bfloat16),
            pltpu.VMEM((2, ROWS, WIDTH), jnp.bfloat16),
            pltpu.SemaphoreType.DMA((2, 24)),
            pltpu.SemaphoreType.DMA((2,)),
            pltpu.SemaphoreType.DMA,
        ],
        input_output_aliases={STAGES + SOURCES + 5: 0, STAGES + SOURCES + 6: 1},
        compiler_params=pltpu.CompilerParams(vmem_limit_bytes=65011712),
        cost_estimate=pl.CostEstimate(
            flops=2 * 2 * ROWS * WIDTH * 5 * WIDTH,
            bytes_accessed=2 * 2 * WIDTH * 5 * WIDTH,
            transcendentals=2 * ROWS * 5 * WIDTH,
        ),
    )(step, info, *inputs, incoming, *mine, *other, gain_in, gain_mid, out, send)


def place_kernel(info_ref, received, out_in, out_ref, sems):
    core = info_ref[8]
    copies = [
        pltpu.make_async_copy(received.at[j], out_ref.at[2 * j + 1 - core], sems.at[j])
        for j in range(SHARE)
    ]
    for copy in copies:
        copy.start()
    for copy in copies:
        copy.wait()


def place(info, received, out):
    return pl.pallas_call(
        place_kernel,
        out_shape=jax.ShapeDtypeStruct(out.shape, out.dtype),
        in_specs=[
            pl.BlockSpec(memory_space=pltpu.SMEM),
            pl.BlockSpec(memory_space=pltpu.VMEM),
            pl.BlockSpec(memory_space=pltpu.HBM),
        ],
        out_specs=pl.BlockSpec(memory_space=pltpu.HBM),
        scratch_shapes=[pltpu.SemaphoreType.DMA((SHARE,))],
        input_output_aliases={2: 0},
        compiler_params=pltpu.CompilerParams(vmem_limit_bytes=8 * 1024 * 1024),
    )(info, received, out)


def lookup_items(item_owner, item_row, table):
    groups = lax.axis_size(DP)
    owner = item_owner.reshape(-1)
    rows = item_row.reshape(-1)
    seq_len = rows.shape[0]
    slots_each = max(2, 2 * seq_len // groups)
    match = (owner[:, None] == jnp.arange(groups, dtype=jnp.int32)[None, :]).astype(jnp.int32)
    earlier = jnp.cumsum(match, axis=0) - match
    slot = jnp.sum(earlier * match, axis=1)
    placed = match[:, :, None] * (
        slot[:, None, None] == jnp.arange(slots_each, dtype=jnp.int32)[None, None, :]
    ).astype(jnp.int32)
    request = jnp.sum(placed * rows[:, None, None], axis=0)
    received = lax.all_to_all(request, DP, split_axis=0, concat_axis=0, tiled=True)
    found = jnp.take(table, received.reshape(-1), axis=0, mode="clip")
    answered = lax.all_to_all(
        found.reshape(groups, slots_each, -1), DP, split_axis=0, concat_axis=0, tiled=True
    )
    flat_rows = answered.reshape(groups * slots_each, table.shape[1])
    return jnp.take(flat_rows, owner * slots_each + slot, axis=0, mode="clip")


def swap(block):
    return lax.ppermute(block, "core", [(0, 1), (1, 0)])


def moved(block, axis, shift):
    size = lax.axis_size(axis)
    return lax.ppermute(block, axis, [(i, (i + shift) % size) for i in range(size)])


ROUND = (0, 1, -1, 2)
LINE = (0, 1, -1, 2, -2, 3, -3, -4)
AROUND = (0, 1, -1, 2, -2, 3, -3, 4)


def ordered_kernel(index, parts, shifts, info_ref, *refs):
    size = len(shifts)
    sources, outs, sems = refs[:size], refs[size:-1], refs[-1]
    each = size // parts
    here = info_ref[index]
    for k, (source, shift) in enumerate(zip(sources, shifts)):
        at = lax.rem(here - shift + size, size)
        for part, out in enumerate(outs):

            @pl.when((at >= part * each) & (at < (part + 1) * each))
            def _():
                pltpu.make_async_copy(source, out.at[at - part * each], sems.at[k]).start()

    for k, source in enumerate(sources):
        pltpu.make_async_copy(source, outs[0].at[0], sems.at[k]).wait()


def ordered(info, index, parts, shifts, sources):
    size = len(shifts)
    block = sources[0].shape
    return pl.pallas_call(
        functools.partial(ordered_kernel, index, parts, shifts),
        out_shape=[jax.ShapeDtypeStruct((size // parts, *block), jnp.bfloat16)] * parts,
        in_specs=[pl.BlockSpec(memory_space=pltpu.SMEM)]
        + [pl.BlockSpec(memory_space=pl.ANY)] * size,
        out_specs=[pl.BlockSpec(memory_space=pltpu.VMEM)] * parts,
        scratch_shapes=[pltpu.SemaphoreType.DMA((size,))],
        compiler_params=pltpu.CompilerParams(vmem_limit_bytes=4 * 1024 * 1024),
    )(info, *sources)


def joined_kernel(*refs):
    sources, (out_ref, sems) = refs[:-2], refs[-2:]
    copies = [
        pltpu.make_async_copy(source, out_ref.at[k], sems.at[k])
        for k, source in enumerate(sources)
    ]
    for copy in copies:
        copy.start()
    for copy in copies:
        copy.wait()


def joined(sources):
    block = sources[0].shape
    return pl.pallas_call(
        joined_kernel,
        out_shape=jax.ShapeDtypeStruct((len(sources), *block), jnp.bfloat16),
        in_specs=[pl.BlockSpec(memory_space=pl.ANY)] * len(sources),
        out_specs=pl.BlockSpec(memory_space=pltpu.VMEM),
        scratch_shapes=[pltpu.SemaphoreType.DMA((len(sources),))],
        compiler_params=pltpu.CompilerParams(vmem_limit_bytes=6 * 1024 * 1024),
    )(*sources)


def swapped(blocks):
    sent = []
    for group in GROUPS:
        if len(group) == 1:
            sent.append(swap(blocks[group[0]]))
        else:
            sent.append(swap(joined([blocks[k] for k in group])))
    return sent


def rings(info, part_a, part_b):
    first, line = {0: part_a}, {0: part_b}
    line[1] = moved(part_b, "dp_1", 1)
    line[-1] = moved(part_b, "dp_1", -1)
    first[1] = moved(part_a, "dp_0", 1)
    first[-1] = moved(part_a, "dp_0", -1)
    line[2] = moved(line[1], "dp_1", 1)
    line[-2] = moved(line[-1], "dp_1", -1)
    first[2] = moved(first[1], "dp_0", 1)
    line[3] = moved(line[2], "dp_1", 1)
    line[-3] = moved(line[-2], "dp_1", -1)
    line[-4] = moved(line[-3], "dp_1", -1)
    column = {0: ordered(info, 10, 1, ROUND, [first[d] for d in ROUND])[0]}
    column[1] = moved(column[0], "dp_1", 1)
    column[-1] = moved(column[0], "dp_1", -1)
    low, high = ordered(info, 11, 2, LINE, [line[d] for d in LINE])
    low_1 = moved(low, "dp_0", 1)
    low_m1 = moved(low, "dp_0", -1)
    high_1 = moved(high, "dp_0", 1)
    high_m1 = moved(high, "dp_0", -1)
    column[2] = moved(column[1], "dp_1", 1)
    column[-2] = moved(column[-1], "dp_1", -1)
    low_2 = moved(low_1, "dp_0", 1)
    high_2 = moved(high_m1, "dp_0", -1)
    column[3] = moved(column[2], "dp_1", 1)
    column[-3] = moved(column[-2], "dp_1", -1)
    column[4] = moved(column[3], "dp_1", 1)
    return [column[d] for d in AROUND] + [low, high, low_1, high_1, low_m1, high_m1, low_2, high_2]


GROUPS = ((8, 9), (0, 1, 2, 3, 4), (10, 12), (5,), (6,), (11, 13), (14,), (15,), (7,))


def empty_kernel(*refs):
    pass


def empty(*shape):
    return pl.pallas_call(
        empty_kernel,
        out_shape=jax.ShapeDtypeStruct(shape, jnp.bfloat16),
        out_specs=pl.BlockSpec(memory_space=pltpu.HBM),
    )()


def program(item_owner, item_row, lengths, table, w_in, w_out, gain_in, gain_mid):
    core = lax.axis_index("core")
    chip = lax.axis_index("chip")
    places = [core, chip, lax.axis_index("dp_0"), lax.axis_index("dp_1")]
    info = jnp.concatenate(
        [lengths[:, 0], jnp.stack(places).astype(jnp.int32), jnp.zeros((4,), jnp.int32)]
    )
    pairs = HEADS // 2
    by_pair = w_in[0].reshape(-1, 4, pairs, PAIR).transpose(0, 2, 1, 3).reshape(-1, 4 * WIDTH)
    part_a = by_pair[:, : SPLIT * WIDTH]
    part_b = jnp.concatenate([by_pair[:, SPLIT * WIDTH :], w_out[0]], axis=1)
    mine = rings(info, part_a, part_b)
    embedded = lookup_items(item_owner, item_row, table)
    inputs = [embedded]
    for k in range(1, STAGES):
        inputs.append(lax.ppermute(embedded, "chip", [(k, 0)]))
    gains = jnp.concatenate([gain_in, gain_mid], axis=0)
    gains_other = swap(gains)
    first = jnp.where(core == 0, gains, gains_other)
    second = jnp.where(core == 0, gains_other, gains)
    scale_in = jnp.stack([first[0], second[0]])
    scale_mid = jnp.stack([first[1], second[1]])
    other = swapped(mine)
    out = empty(2 * SHARE, ROWS, WIDTH)
    send = empty(SHARE, ROWS, WIDTH)
    steps = SHARE + 2 * (STAGES - 1)
    blank = empty(ROWS, WIDTH)
    forward = [(i, i + 1) for i in range(STAGES - 1)]

    def two_steps(turn, carry):
        out, send, result, incoming = carry
        for step in (2 * turn, 2 * turn + 1):
            arriving = lax.ppermute(result, "chip", forward)
            out, send, result = stage(
                step.reshape(1), info, inputs, incoming, mine, other, scale_in, scale_mid, out, send
            )
            incoming = arriving
        return (out, send, result, incoming)

    out, send, _, _ = lax.fori_loop(0, steps // 2, two_steps, (out, send, blank, blank))
    out = place(info, swap(send), out)
    return out[None, None]


def solution(mesh):
    split = Mesh(mesh.devices.reshape(STAGES, 2, 4, 8), ("chip", "core", "dp_0", "dp_1"))
    placed = (
        P(ALL, DP, None, None),
        P(ALL, DP, None),
        P(None, DP),
        P(DP, None),
        P(ALL, DP, None),
        P(ALL, DP, None),
        P(ALL, None),
        P(ALL, None),
    )
    return jax.shard_map(
        program,
        mesh=split,
        in_specs=placed,
        out_specs=P(ALL, DP, None, None, None),
        check_vma=False,
    )
```
